128 devices in a mesh: row: 16 (over x, y), col: 8 (over z, core).
Axes of the slice: x: 4, y: 4, z: 4, core: 2. Of those that a mesh axis runs over, the one named last changes fastest.
Arguments:
- weights: int32 [8192, 8192], P('row', 'col'), may hold values from 1 to 64
Outputs:
- distances: int32 [8192, 8192], P('row', 'col')
The draws below stay inside these ranges and needn't reach their ends.
All inputs are finite; a program needn't handle non-finite values.
Results may differ from the reference program's by a relative error of at most 0.000001.
Values may be sent and summed in bfloat16 or wider, within the bound.
No kernel may reach another device: no remote copies, remote signals or barrier semaphores. Data moves between devices by JAX's collectives and lax.ppermute only.
A program may use at most 64 MiB of HBM per device.

```python
import jax
import jax.numpy as jnp
from jax import lax

PIVOT = 128
STEPS = 4
VERTS = 8192
STRIDE = 2048


def set_ends(drawn, rng, low, top_value):
    shape = drawn.shape
    place = [jax.random.randint(jax.random.fold_in(rng, axis), (), 0, shape[axis]) for axis in range(len(shape))]
    drawn = drawn.at[tuple(place)].set(low)
    longest = shape.index(max(shape))
    place[longest] = (place[longest] + 1) % shape[longest]
    return drawn.at[tuple(place)].set(top_value)


def setup_inputs(seed: int = 0) -> dict:
    splits = jax.random.split(jax.random.key(seed), 2)
    weights = set_ends(jax.random.randint(splits[0], (VERTS, VERTS), 1, 65), jax.random.fold_in(splits[0], 1), 1, 64).astype(jnp.int32)
    return {"weights": weights}


def relax(vertex, dist):
    vertex = jnp.asarray(vertex).astype(jnp.int32)
    column = lax.dynamic_slice_in_dim(dist, vertex, 1, 1)
    across = lax.dynamic_slice_in_dim(dist, vertex, 1, 0)
    return jnp.minimum(dist, column + across)


def reference(weights):
    labels = jnp.arange(VERTS, dtype=jnp.int32)
    dist = jnp.where(labels[:, None] == labels[None, :], jnp.int32(0), weights).astype(jnp.int32)
    for step in range(STEPS):
        first = step * STRIDE
        dist = lax.fori_loop(first, first + PIVOT, relax, dist)
    return dist
```

```python
import jax
import jax.numpy as jnp
from jax import lax
from jax.experimental import pallas as pl
from jax.experimental.pallas import tpu as pltpu
from jax.sharding import PartitionSpec as P

PIVOT = 128
STEPS = 4
SIDE = 4
F32, BF16 = jnp.float32, jnp.bfloat16
RATE = 8.0625
LN2 = 0.6931471805599453
SLACK = 0.004
LEFT, RIGHT = 6, 7
LINE = [[SIDE * i + k for k in range(SIDE)] for i in range(SIDE)]
COLUMN = [[SIDE * k + i for k in range(SIDE)] for i in range(SIDE)]
COL_LINE = [[2 * k + c for k in range(SIDE)] for c in range(2)]
PAIR = [[2 * k, 2 * k + 1] for k in range(SIDE)]


def encode(value):
    a = jnp.maximum(value.astype(F32) - 1.0, 0.0)
    a = jnp.where(a >= 32.0, a - 32.0, a)
    scale = jnp.exp2(125.0 - RATE * a).astype(BF16)
    zero = jnp.zeros_like(scale)
    far = value >= 33.0
    lo = jnp.where(far, zero, scale)
    hi = jnp.where(far, scale, zero)
    mid = jnp.where(value >= 17.0, lo, zero)
    t1 = lo * BF16(2.0**-66)
    t4 = t1 * BF16(2.0**-62)
    t5 = hi * BF16(2.0**-11)
    t3 = t5 * BF16(2.0**-119)
    return t1, lo, t3, t4, t5, mid


def encode_left(value):
    t1, t2, t3, t4, t5, mid = encode(value)
    return t1, t4, t3, t2, t5, mid * BF16(2.0**124)


def encode_right(value):
    t1, t2, t3, t4, t5, mid = encode(value)
    return t1, t3, t4, t2, t5, t2, mid * BF16(2.0**123)


def decode(s1, s2, s3):
    r = jnp.log(s1) - 118.0 * LN2
    r = jnp.maximum(r, jnp.minimum(jnp.log(s2), 128.0 * LN2) - 250.0 * LN2)
    r = jnp.maximum(r, jnp.minimum(jnp.log(s3), 128.0 * LN2) - 497.0 * LN2)
    return 2.0 - jnp.floor(r * (1.0 / (RATE * LN2)) + SLACK)


def dot(left, right):
    return jnp.dot(left, right, preferred_element_type=F32)


def windows(left_ref, right_ref, sums_ref, slot, k, rows, cols):
    sums_ref[slot, :rows, cols] = dot(left_ref[:rows, :k], right_ref[:k, cols])
    sums_ref[slot + 1, :rows, cols] = dot(left_ref[:rows, k : 4 * k], right_ref[k : 4 * k, cols])
    sums_ref[slot + 2, :rows, cols] = dot(left_ref[:rows, 3 * k : 6 * k], right_ref[4 * k : 7 * k, cols])


def put_left(left_ref, source, k, rows, step=64):
    def body(i, _):
        at = pl.ds(pl.multiple_of(i * step, step), step)
        for t, table in enumerate(encode_left(source(at))):
            left_ref[at, t * k : (t + 1) * k] = table
        return 0

    lax.fori_loop(0, rows // step, body, 0)


def put_right(right_ref, source, k, rows, step=32):
    def body(i, _):
        at = pl.multiple_of(i * step, step)
        for t, table in enumerate(encode_right(source(pl.ds(at, step)))):
            right_ref[pl.ds(t * k + at, step), :] = table
        return 0

    lax.fori_loop(0, rows // step, body, 0)


def closure_kernel(index_ref, *refs):
    size = STEPS * PIVOT
    panels, blocks = refs[:SIDE], refs[SIDE : 2 * SIDE]
    out_ref, own_ref, x_ref, left_ref, right_ref, left2_ref, right2_ref, sums_ref = refs[2 * SIDE :]
    ix, iz = index_ref[0], index_ref[2]
    for shift in range(SIDE):
        col = pl.multiple_of(lax.rem(iz + SIDE - shift, SIDE) * PIVOT, PIVOT)
        own_ref[:, pl.ds(col, PIVOT)] = panels[shift][...]
        for other in range(SIDE):
            row = pl.multiple_of(lax.rem(ix + SIDE - other, SIDE) * PIVOT, PIVOT)
            x_ref[pl.ds(row, PIVOT), pl.ds(col, PIVOT)] = blocks[shift][other]

    def step(s, _):
        at = pl.ds(pl.multiple_of(s * PIVOT, PIVOT), PIVOT)
        d = x_ref[at, at].astype(F32)
        for v in range(PIVOT):
            d = jnp.minimum(d, d[:, v : v + 1] + d[v : v + 1, :])
        left_ref[:PIVOT, :] = jnp.concatenate(encode_left(d.astype(BF16)), axis=1)
        put_right(right_ref, lambda r: x_ref[pl.ds(s * PIVOT + r.start, r.size), :], PIVOT, PIVOT)
        for half in range(2):
            windows(left_ref, right_ref, sums_ref, 0, PIVOT, PIVOT, slice(256 * half, 256 * (half + 1)))

        def close_rows(i, _):
            row = pl.ds(pl.multiple_of(i * 32, 32), 32)
            new = decode(sums_ref[0, row, :], sums_ref[1, row, :], sums_ref[2, row, :])
            to = pl.ds(pl.multiple_of(s * PIVOT + i * 32, 32), 32)
            x_ref[to, :] = jnp.minimum(x_ref[to, :].astype(F32), new).astype(BF16)
            return 0

        put_left(left_ref, lambda r: x_ref[r, at], PIVOT, size)
        lax.fori_loop(0, PIVOT // 32, close_rows, 0)
        put_right(right_ref, lambda r: x_ref[pl.ds(s * PIVOT + r.start, r.size), :], PIVOT, PIVOT)
        for half in range(2):
            windows(left_ref, right_ref, sums_ref, 0, PIVOT, size, slice(256 * half, 256 * (half + 1)))

        def relax(i, _):
            row = pl.ds(pl.multiple_of(i * 32, 32), 32)
            new = decode(sums_ref[0, row, :], sums_ref[1, row, :], sums_ref[2, row, :])
            x_ref[row, :] = jnp.minimum(x_ref[row, :].astype(F32), new).astype(BF16)
            return 0

        lax.fori_loop(0, size // 32, relax, 0)
        return 0

    lax.fori_loop(0, STEPS, step, 0)

    k = 2 * PIVOT
    for chunk in range(2):
        cols = slice(chunk * k, (chunk + 1) * k)
        put_left(left2_ref, lambda r: own_ref[r, cols], k, size)
        put_right(right2_ref, lambda r: x_ref[pl.ds(chunk * k + r.start, r.size), :], k, k)
        for half in range(2):
            windows(left2_ref, right2_ref, sums_ref, 3 * chunk, k, size, slice(256 * half, 256 * (half + 1)))

    def finish(i, _):
        row = pl.ds(pl.multiple_of(i * 32, 32), 32)
        new = decode(*(jnp.maximum(sums_ref[w, row, :], sums_ref[3 + w, row, :]) for w in range(3)))
        out_ref[row, :] = jnp.minimum(own_ref[row, :].astype(F32), new).astype(BF16)
        return 0

    lax.fori_loop(0, size // 32, finish, 0)


def final_kernel(index_ref, own_ref, *refs):
    pieces = refs[:SIDE]
    weights_ref, out_ref, left_ref, right_ref, sums_ref = refs[SIDE:]
    k = 2 * PIVOT
    rows, width = weights_ref.shape
    tile = pl.program_id(0)

    @pl.when(tile == 0)
    def _():
        for chunk in range(2):
            put_left(
                left_ref.at[chunk], lambda r: own_ref[r, chunk * k : (chunk + 1) * k], k, rows
            )

    part = PIVOT // SIDE
    for shift in range(SIDE):
        for other in range(SIDE):
            s = lax.rem(index_ref[0] + SIDE - other, SIDE)
            q = lax.rem(index_ref[1] + SIDE - shift, SIDE)
            base = (s // 2) * (RIGHT * k) + lax.rem(s, 2) * PIVOT + q * part
            for t, table in enumerate(encode_right(pieces[shift][other])):
                right_ref[pl.ds(pl.multiple_of(base + t * k, part), part), :] = table
    for chunk in range(2):
        windows(
            left_ref.at[chunk],
            right_ref.at[chunk * RIGHT * k : (chunk + 1) * RIGHT * k],
            sums_ref,
            3 * chunk,
            k,
            rows,
            slice(0, width),
        )
    diagonal = index_ref[3] - tile * width

    def finish(i, _):
        row = pl.ds(pl.multiple_of(i * 32, 32), 32)
        new = decode(*(jnp.maximum(sums_ref[w, row, :], sums_ref[3 + w, row, :]) for w in range(3)))
        best = jnp.minimum(weights_ref[row, :].astype(F32), new).astype(jnp.int32)
        down = lax.broadcasted_iota(jnp.int32, best.shape, 0) + (diagonal + i * 32)
        across = lax.broadcasted_iota(jnp.int32, best.shape, 1)
        out_ref[row, :] = jnp.where(down == across, 0, best)
        return 0

    lax.fori_loop(0, rows // 32, finish, 0)


def rotate(array, axis, lines, shift):
    pairs = [(line[i], line[(i + shift) % SIDE]) for line in lines for i in range(SIDE)]
    return lax.ppermute(array, axis, pairs)


def gather_line(array, axis, lines):
    return [array] + [rotate(array, axis, lines, shift) for shift in (1, 3, 2)]


def in_order(parts):
    return [parts[0], parts[1], parts[3], parts[2]]


def per_device(weights):
    rows, cols = weights.shape
    part = PIVOT // SIDE
    row, col = lax.axis_index("row"), lax.axis_index("col")
    index = jnp.stack([row // SIDE, row % SIDE, col // 2, row * rows - col * cols]).astype(jnp.int32)
    panel = weights[:, :PIVOT].astype(BF16)
    strip = weights[:PIVOT, :].astype(BF16)
    panel = lax.all_gather(panel, "col", axis_index_groups=PAIR)[0]
    block = panel[:PIVOT].reshape(SIDE * SIDE, cols)
    message = jnp.concatenate([strip[:part], block])
    for y in range(1, SIDE):
        sent = jnp.concatenate([strip[y * part : (y + 1) * part], block])
        got = lax.ppermute(sent, "row", [(line[0], line[y]) for line in LINE])
        message = jnp.where(row % SIDE == y, got, message)
    along_x = in_order(gather_line(message, "row", COLUMN))
    quarters = jnp.stack([m[:part] for m in along_x])
    blocks = jnp.stack([m[part:].reshape(PIVOT, PIVOT) for m in along_x])
    panels = in_order(gather_line(panel, "col", COL_LINE))
    block_list = in_order(gather_line(blocks, "col", COL_LINE))
    pieces = in_order(gather_line(quarters, "row", LINE))

    size = STEPS * PIVOT
    smem = pl.BlockSpec(memory_space=pltpu.SMEM)
    vmem = pl.BlockSpec(memory_space=pltpu.VMEM)
    own = pl.pallas_call(
        closure_kernel,
        out_shape=jax.ShapeDtypeStruct((rows, size), BF16),
        in_specs=[smem] + [vmem] * (2 * SIDE),
        out_specs=vmem,
        scratch_shapes=[
            pltpu.VMEM((rows, size), BF16),
            pltpu.VMEM((size, size), BF16),
            pltpu.VMEM((size, LEFT * PIVOT), BF16),
            pltpu.VMEM((RIGHT * PIVOT, size), BF16),
            pltpu.VMEM((rows, LEFT * 2 * PIVOT), BF16),
            pltpu.VMEM((RIGHT * 2 * PIVOT, size), BF16),
            pltpu.VMEM((6, rows, size), F32),
        ],
        cost_estimate=pl.CostEstimate(flops=20_000_000_000, bytes_accessed=2_000_000, transcendentals=0),
        name="closure",
    )(index, *panels, *block_list)

    width = 256
    k = 2 * PIVOT
    return pl.pallas_call(
        final_kernel,
        grid=(cols // width,),
        out_shape=jax.ShapeDtypeStruct((rows, cols), jnp.int32),
        in_specs=[smem, pl.BlockSpec((rows, size), lambda j: (0, 0))]
        + [pl.BlockSpec((SIDE, part, width), lambda j: (0, 0, j))] * SIDE
        + [pl.BlockSpec((rows, width), lambda j: (0, j))],
        out_specs=pl.BlockSpec((rows, width), lambda j: (0, j)),
        scratch_shapes=[
            pltpu.VMEM((2, rows, LEFT * k), BF16),
            pltpu.VMEM((2 * RIGHT * k, width), BF16),
            pltpu.VMEM((6, rows, width), F32),
        ],
        cost_estimate=pl.CostEstimate(flops=4_000_000_000, bytes_accessed=6_000_000, transcendentals=0),
        name="final",
    )(index, own, *pieces, weights)


def solution(mesh):
    placed = (P("row", "col"),)
    return jax.shard_map(
        per_device, mesh=mesh, in_specs=placed, out_specs=P("row", "col"), check_vma=False
    )
```

```python
import jax
import jax.numpy as jnp
from jax import lax
from jax.experimental import pallas as pl
from jax.experimental.pallas import tpu as pltpu
from jax.sharding import PartitionSpec as P

PIVOT = 128
STEPS = 4
SIDE = 4
HALF = 2 * PIVOT
SIZE = STEPS * PIVOT
PART = PIVOT // SIDE
F32, BF16 = jnp.float32, jnp.bfloat16
RATE = 8.0625
LN2 = 0.6931471805599453
SLACK = 0.004
LEFT, RIGHT = 6, 7
SQUARINGS = 6
LINE = [[SIDE * i + k for k in range(SIDE)] for i in range(SIDE)]
COLUMN = [[SIDE * k + i for k in range(SIDE)] for i in range(SIDE)]
COL_LINE = [[2 * k + c for k in range(SIDE)] for c in range(2)]
PAIR = [[2 * k, 2 * k + 1] for k in range(SIDE)]


def encode(value):
    far = value >= BF16(33.0)
    a = value - jnp.where(far, BF16(33.0), BF16(1.0))
    scale = jnp.exp2(BF16(125.0) - BF16(8.0) * a) * jnp.exp2(BF16(-0.0625) * a)
    zero = jnp.zeros_like(scale)
    lo = jnp.where(far, zero, scale)
    t5 = jnp.where(far, scale * BF16(2.0**-11), zero)
    mid = jnp.where(value >= BF16(17.0), lo, zero)
    t1 = lo * BF16(2.0**-66)
    t4 = t1 * BF16(2.0**-62)
    t3 = t5 * BF16(2.0**-119)
    return t1, lo, t3, t4, t5, mid


def left_tables(tables):
    t1, t2, t3, t4, t5, mid = tables
    return t1, t4, t3, t2, t5, mid * BF16(2.0**124)


def right_tables(tables):
    t1, t2, t3, t4, t5, mid = tables
    return t1, t3, t4, t2, t5, t2, mid * BF16(2.0**123)


def decode(s1, s2, s3):
    near = s1 >= 2.0**-59.4
    middle = s2 >= 2.0**-121
    s = jnp.where(near, s1, jnp.where(middle, s2, s3))
    p1, p2, p3 = (p / RATE - SLACK + 2.0 for p in (118.0, 250.0, 497.0))
    p = jnp.where(near, p1, jnp.where(middle, p2, p3))
    return jnp.ceil(p - jnp.log(s) * (1.0 / (RATE * LN2)))


def dot(left, right):
    return jnp.dot(left, right, preferred_element_type=F32)


def put_left(left_ref, at, tables):
    for t, table in enumerate(left_tables(tables)):
        left_ref[at, t * HALF : (t + 1) * HALF] = table


def put_right(right_ref, at, size, tables):
    for t, table in enumerate(right_tables(tables)):
        right_ref[pl.ds(t * HALF + at, size), :] = table


def sums(left_ref, right_ref, rows, cols):
    return (
        dot(left_ref[rows, :HALF], right_ref[:HALF, cols]),
        dot(left_ref[rows, HALF : 4 * HALF], right_ref[HALF : 4 * HALF, cols]),
        dot(left_ref[rows, 3 * HALF : 6 * HALF], right_ref[4 * HALF : 7 * HALF, cols]),
    )


CHUNK = 32


def lower(ref, rows, cols, windows):
    for i in range(0, windows[0].shape[0], CHUNK):
        at = slice(rows + i, rows + i + CHUNK)
        new = decode(*(w[i : i + CHUNK] for w in windows))
        ref[at, cols] = jnp.minimum(ref[at, cols].astype(F32), new).astype(BF16)


def encode_rows(ref, rows, cols, count, left=None, right=None):
    for i in range(0, count, CHUNK):
        tables = encode(ref[rows + i : rows + i + CHUNK, cols])
        if left is not None:
            put_left(left, slice(i, i + CHUNK), tables)
        if right is not None:
            put_right(right, i, CHUNK, tables)


def close(x_ref, at, left_ref, right_ref):
    cols = slice(at, at + HALF)

    def square(_, carry):
        encode_rows(x_ref, at, cols, HALF, left_ref, right_ref)
        lower(x_ref, at, cols, sums(left_ref, right_ref, slice(0, HALF), slice(0, HALF)))
        return carry

    lax.fori_loop(0, SQUARINGS, square, 0)


def multiply(ref, cols, source, source_cols, left_ref, right_ref, first, count):
    for r in range(first, first + count, HALF):
        encode_rows(source, r, source_cols, HALF, left=left_ref)
        lower(ref, r, cols, sums(left_ref, right_ref, slice(0, HALF), slice(0, HALF)))


P_, Q_ = slice(0, HALF), slice(HALF, SIZE)


def closure_kernel(index_ref, *refs):
    blocks = refs[:SIDE]
    x_ref, left_ref, right_ref = refs[SIDE:]
    for shift in range(SIDE):
        col = pl.multiple_of(lax.rem(index_ref[2] + SIDE - shift, SIDE) * PIVOT, PIVOT)
        for other in range(SIDE):
            row = pl.multiple_of(lax.rem(index_ref[0] + SIDE - other, SIDE) * PIVOT, PIVOT)
            x_ref[pl.ds(row, PIVOT), pl.ds(col, PIVOT)] = blocks[shift][other]
    close(x_ref, 0, left_ref, right_ref)
    encode_rows(x_ref, 0, P_, HALF, right=right_ref)
    multiply(x_ref, P_, x_ref, P_, left_ref, right_ref, HALF, HALF)
    encode_rows(x_ref, 0, Q_, HALF, right=right_ref)
    multiply(x_ref, Q_, x_ref, P_, left_ref, right_ref, HALF, HALF)
    close(x_ref, HALF, left_ref, right_ref)


def chain_kernel(index_ref, x_ref, *refs):
    panels = refs[:SIDE]
    own_ref, left_ref, right_ref = refs[SIDE:]
    rows = own_ref.shape[0]
    for shift in range(SIDE):
        col = pl.multiple_of(lax.rem(index_ref[2] + SIDE - shift, SIDE) * PIVOT, PIVOT)
        own_ref[:, pl.ds(col, PIVOT)] = panels[shift][...]
    for at, cols, to, source in ((0, P_, P_, P_), (0, Q_, Q_, P_), (HALF, Q_, Q_, Q_), (HALF, P_, P_, Q_)):
        encode_rows(x_ref, at, cols, HALF, right=right_ref)
        multiply(own_ref, to, own_ref, source, left_ref, right_ref, 0, rows)


def final_kernel(index_ref, own_ref, *refs):
    pieces = refs[:SIDE]
    weights_ref, out_ref, left_ref, right_ref = refs[SIDE:]
    rows, width = weights_ref.shape
    tile = pl.program_id(0)

    @pl.when(tile == 0)
    def _():
        for chunk in range(2):
            encode_rows(own_ref, 0, slice(chunk * HALF, (chunk + 1) * HALF), rows, left=left_ref.at[chunk])

    for shift in range(SIDE):
        for other in range(SIDE):
            s = lax.rem(index_ref[0] + SIDE - other, SIDE)
            q = lax.rem(index_ref[1] + SIDE - shift, SIDE)
            base = (s // 2) * (RIGHT * HALF) + lax.rem(s, 2) * PIVOT + q * PART
            for t, table in enumerate(right_tables(encode(pieces[shift][other]))):
                right_ref[pl.ds(pl.multiple_of(base + t * HALF, PART), PART), :] = table
    diagonal = index_ref[3] - tile * width
    for r in range(0, rows, HALF):
        parts = [
            sums(
                left_ref.at[chunk],
                right_ref.at[chunk * RIGHT * HALF : (chunk + 1) * RIGHT * HALF],
                slice(r, r + HALF),
                slice(0, width),
            )
            for chunk in range(2)
        ]
        for i in range(0, HALF, CHUNK):
            row = slice(r + i, r + i + CHUNK)
            new = decode(*(jnp.maximum(a[i : i + CHUNK], b[i : i + CHUNK]) for a, b in zip(*parts)))
            best = jnp.minimum(weights_ref[row, :].astype(F32), new).astype(jnp.int32)
            down = lax.broadcasted_iota(jnp.int32, best.shape, 0)
            across = lax.broadcasted_iota(jnp.int32, best.shape, 1)
            out_ref[row, :] = jnp.where(across - down == diagonal + (r + i), 0, best)


SMEM = pl.BlockSpec(memory_space=pltpu.SMEM)
VMEM = pl.BlockSpec(memory_space=pltpu.VMEM)


def cost(flops):
    return pl.CostEstimate(flops=flops, bytes_accessed=2_000_000, transcendentals=0)


def closure_call(index, blocks):
    return pl.pallas_call(
        closure_kernel,
        out_shape=jax.ShapeDtypeStruct((SIZE, SIZE), BF16),
        in_specs=[SMEM] + [VMEM] * SIDE,
        out_specs=VMEM,
        scratch_shapes=[pltpu.VMEM((HALF, LEFT * HALF), BF16), pltpu.VMEM((RIGHT * HALF, HALF), BF16)],
        cost_estimate=cost(10_000_000_000),
        name="closure",
    )(index, *blocks)


def chain_call(index, x, panels):
    rows = panels[0].shape[0]
    return pl.pallas_call(
        chain_kernel,
        out_shape=jax.ShapeDtypeStruct((rows, SIZE), BF16),
        in_specs=[SMEM, VMEM] + [VMEM] * SIDE,
        out_specs=VMEM,
        scratch_shapes=[pltpu.VMEM((HALF, LEFT * HALF), BF16), pltpu.VMEM((RIGHT * HALF, HALF), BF16)],
        cost_estimate=cost(4_000_000_000),
        name="chain",
    )(index, x, *panels)


def final_call(index, own, pieces, weights, width=256):
    rows, cols = weights.shape
    return pl.pallas_call(
        final_kernel,
        grid=(cols // width,),
        out_shape=jax.ShapeDtypeStruct((rows, cols), jnp.int32),
        in_specs=[SMEM, pl.BlockSpec((rows, SIZE), lambda j: (0, 0))]
        + [pl.BlockSpec((SIDE, PART, width), lambda j: (0, 0, j))] * SIDE
        + [pl.BlockSpec((rows, width), lambda j: (0, j))],
        out_specs=pl.BlockSpec((rows, width), lambda j: (0, j)),
        scratch_shapes=[
            pltpu.VMEM((2, rows, LEFT * HALF), BF16),
            pltpu.VMEM((2 * RIGHT * HALF, width), BF16),
        ],
        cost_estimate=cost(4_000_000_000),
        name="final",
    )(index, own, *pieces, weights)


def gather_line(array, axis, lines):
    got = {0: array}
    for shift in (1, 3, 2):
        pairs = [(line[i], line[(i + shift) % SIDE]) for line in lines for i in range(SIDE)]
        got[shift] = lax.ppermute(array, axis, pairs)
    return [got[shift] for shift in range(SIDE)]


def per_device(weights):
    rows, cols = weights.shape
    row, col = lax.axis_index("row"), lax.axis_index("col")
    index = jnp.stack([row // SIDE, row % SIDE, col // 2, row * rows - col * cols]).astype(jnp.int32)
    panel = weights[:, :PIVOT].astype(BF16)
    strip = weights[:PIVOT, :].astype(BF16)
    panel = lax.all_gather(panel, "col", axis_index_groups=PAIR)[0]
    block = panel[:PIVOT].reshape(SIDE * SIDE, cols)
    message = jnp.concatenate([strip[:PART], block])
    for y in range(1, SIDE):
        sent = jnp.concatenate([strip[y * PART : (y + 1) * PART], block])
        got = lax.ppermute(sent, "row", [(line[0], line[y]) for line in LINE])
        message = jnp.where(row % SIDE == y, got, message)
    panels = gather_line(panel, "col", COL_LINE)
    along_x = gather_line(message, "row", COLUMN)
    quarters = jnp.stack([m[:PART] for m in along_x])
    blocks = jnp.stack([m[PART:].reshape(PIVOT, PIVOT) for m in along_x])
    blocks = gather_line(blocks, "col", COL_LINE)
    pieces = gather_line(quarters, "row", LINE)
    x = closure_call(index, blocks)
    own = chain_call(index, x, panels)
    return final_call(index, own, pieces, weights)


def solution(mesh):
    placed = (P("row", "col"),)
    return jax.shard_map(
        per_device, mesh=mesh, in_specs=placed, out_specs=P("row", "col"), check_vma=False
    )
```

```python
import jax
import jax.numpy as jnp
from jax import lax
from jax.experimental import pallas as pl
from jax.experimental.pallas import tpu as pltpu
from jax.sharding import PartitionSpec as P

PIVOT = 128
STEPS = 4
SIDE = 4
HALF = 2 * PIVOT
SIZE = STEPS * PIVOT
PART = PIVOT // SIDE
F32, BF16 = jnp.float32, jnp.bfloat16
RATE = 8.0625
LN2 = 0.6931471805599453
SLACK = 0.004
TABLES = 6
SQUARINGS = 6
LINE = [[SIDE * i + k for k in range(SIDE)] for i in range(SIDE)]
COLUMN = [[SIDE * k + i for k in range(SIDE)] for i in range(SIDE)]
COL_LINE = [[2 * k + c for k in range(SIDE)] for c in range(2)]
PAIR = [[2 * k, 2 * k + 1] for k in range(SIDE)]


def encode(value):
    far = value >= BF16(33.0)
    a = value - jnp.where(far, BF16(33.0), BF16(1.0))
    scale = jnp.exp2(BF16(125.0) - BF16(8.0) * a) * jnp.exp2(BF16(-0.0625) * a)
    zero = jnp.zeros_like(scale)
    lo = jnp.where(far, zero, scale)
    t5 = jnp.where(far, scale * BF16(2.0**-12), zero)
    mid = jnp.where(value >= BF16(17.0), lo, zero)
    t1 = lo * BF16(2.0**-66)
    t4 = t1 * BF16(2.0**-62)
    t3 = t5 * BF16(2.0**-118)
    return t1, lo, t3, t4, t5, mid * BF16(2.0**123)


def decode(s1, s2, s3):
    near = s1 >= 2.0**-59.4
    middle = s2 >= 2.0**-121
    s = jnp.where(near, s1, jnp.where(middle, s2, s3))
    p1, p2, p3 = (p / RATE - SLACK + 2.0 for p in (118.0, 250.0, 496.0))
    p = jnp.where(near, p1, jnp.where(middle, p2, p3))
    return jnp.ceil(p - jnp.log(s) * (1.0 / (RATE * LN2)))


def dot(left, right):
    return jnp.dot(left, right, preferred_element_type=F32)


CHUNK = 32


def sums(left, right, rows, cols):
    def l(*tables):
        return jnp.concatenate([left[t, rows, :] for t in tables], axis=1)

    def r(*tables):
        return jnp.concatenate([right[t, :, cols] for t in tables], axis=0)

    return dot(l(0), r(0)), dot(l(3, 2, 1), r(2, 3, 1)), dot(l(1, 4, 5), r(4, 1, 5))


def lower(ref, rows, cols, windows):
    for i in range(0, windows[0].shape[0], CHUNK):
        at = slice(rows + i, rows + i + CHUNK)
        new = decode(*(w[i : i + CHUNK] for w in windows))
        ref[at, cols] = jnp.minimum(ref[at, cols].astype(F32), new).astype(BF16)


def encode_rows(ref, rows, cols, count, to):
    for i in range(0, count, CHUNK):
        for t, table in enumerate(encode(ref[rows + i : rows + i + CHUNK, cols])):
            to[t, i : i + CHUNK, :] = table


ALL = slice(0, HALF)
P_, Q_ = slice(0, HALF), slice(HALF, SIZE)


def close(x_ref, at, tab_ref):
    cols = slice(at, at + HALF)

    def square(_, carry):
        encode_rows(x_ref, at, cols, HALF, tab_ref)
        lower(x_ref, at, cols, sums(tab_ref, tab_ref, ALL, ALL))
        return carry

    lax.fori_loop(0, SQUARINGS, square, 0)
    encode_rows(x_ref, at, cols, HALF, tab_ref)


def multiply(ref, cols, source, source_cols, left_ref, right_ref, first, count):
    for n, r in enumerate(range(first, first + count, HALF)):
        left = left_ref.at[n]
        encode_rows(source, r, source_cols, HALF, left)
        lower(ref, r, cols, sums(left, right_ref, ALL, ALL))


def place(shift, axis_position):
    return pl.multiple_of(lax.rem(axis_position + SIDE - shift, SIDE) * PIVOT, PIVOT)


def chain_kernel(*refs):
    blocks, panels = refs[:SIDE], refs[SIDE : 2 * SIDE]
    own_ref, x_ref, left_ref, right_ref, tab_ref, block_sem, panel_sem = refs[2 * SIDE :]
    rows = own_ref.shape[0]
    ix, iz = lax.axis_index("row") // SIDE, lax.axis_index("col") // 2
    block_copies, panel_copies = [], []
    for shift in range(SIDE):
        col = pl.ds(place(shift, iz), PIVOT)
        for other in range(SIDE):
            to = x_ref.at[pl.ds(place(other, ix), PIVOT), col]
            block_copies.append(pltpu.make_async_copy(blocks[shift].at[other], to, block_sem.at[shift, other]))
        panel_copies.append(pltpu.make_async_copy(panels[shift], own_ref.at[:, col], panel_sem.at[shift]))
    for copy in block_copies + panel_copies:
        copy.start()
    for copy in block_copies:
        copy.wait()
    close(x_ref, 0, tab_ref)
    multiply(x_ref, P_, x_ref, P_, left_ref, tab_ref, HALF, HALF)
    encode_rows(x_ref, 0, Q_, HALF, right_ref)
    multiply(x_ref, Q_, x_ref, P_, left_ref, right_ref, HALF, HALF)
    for copy in panel_copies:
        copy.wait()
    multiply(own_ref, P_, own_ref, P_, left_ref, tab_ref, 0, rows)
    multiply(own_ref, Q_, own_ref, P_, left_ref, right_ref, 0, rows)
    close(x_ref, HALF, tab_ref)
    multiply(own_ref, Q_, own_ref, Q_, left_ref, tab_ref, 0, rows)
    encode_rows(x_ref, HALF, P_, HALF, right_ref)
    multiply(own_ref, P_, own_ref, Q_, left_ref, right_ref, 0, rows)


def final_kernel(own_ref, *refs):
    pieces = refs[:SIDE]
    weights_hbm, out_hbm, left_ref, right_ref, pivot_ref, sums_ref, weights_ref, out_ref, sem, in_sem, out_sem = refs[SIDE:]
    rows, total = weights_ref.shape
    row, col = lax.axis_index("row"), lax.axis_index("col")
    tiles = [slice(c, c + HALF) for c in range(0, total, HALF)]
    copies, loads, stores = [], [], []
    for shift in range(SIDE):
        q = lax.rem(row % SIDE + SIDE - shift, SIDE) * PART
        for other in range(SIDE):
            at = pl.multiple_of(place(other, row // SIDE) + q, PART)
            to = pivot_ref.at[pl.ds(at, PART), :]
            copies.append(pltpu.make_async_copy(pieces[shift].at[other], to, sem.at[shift, other]))
    for n, cols in enumerate(tiles):
        loads.append(pltpu.make_async_copy(weights_hbm.at[:, cols], weights_ref.at[:, cols], in_sem.at[n]))
        stores.append(pltpu.make_async_copy(out_ref.at[:, cols], out_hbm.at[:, cols], out_sem.at[n]))
    for copy in copies + loads:
        copy.start()
    for chunk in range(2):
        encode_rows(own_ref, 0, slice(chunk * HALF, (chunk + 1) * HALF), rows, left_ref.at[chunk])
    for copy in copies:
        copy.wait()

    def finish(n, r, slot):
        if r == 0:
            loads[n].wait()
        diagonal = row * rows + r - col * total - tiles[n].start
        for i in range(0, HALF, CHUNK):
            at, to = slice(i, i + CHUNK), slice(r + i, r + i + CHUNK)
            new = decode(*(jnp.maximum(sums_ref[slot, 0, w, at, :], sums_ref[slot, 1, w, at, :]) for w in range(3)))
            best = jnp.minimum(weights_ref[to, tiles[n]].astype(F32), new).astype(jnp.int32)
            down = lax.broadcasted_iota(jnp.int32, best.shape, 0)
            across = lax.broadcasted_iota(jnp.int32, best.shape, 1)
            out_ref[to, tiles[n]] = jnp.where(across - down == diagonal + i, 0, best)
        if r + HALF == rows:
            stores[n].start()

    units = [(n, r) for n in range(len(tiles)) for r in range(0, rows, HALF)]
    for u, (n, r) in enumerate(units):
        if r == 0:
            for chunk in range(2):
                encode_rows(pivot_ref, chunk * HALF, tiles[n], HALF, right_ref.at[n % 2, chunk])
        for chunk in range(2):
            at = slice(r, r + HALF)
            for w, value in enumerate(sums(left_ref.at[chunk], right_ref.at[n % 2, chunk], at, ALL)):
                sums_ref[u % 2, chunk, w] = value
        if u:
            finish(*units[u - 1], (u - 1) % 2)
    finish(*units[-1], (len(units) - 1) % 2)
    for copy in stores:
        copy.wait()


VMEM = pl.BlockSpec(memory_space=pltpu.VMEM)
ANY = pl.BlockSpec(memory_space=pl.ANY)


def cost(flops):
    return pl.CostEstimate(flops=flops, bytes_accessed=2_000_000, transcendentals=0)


def chain_call(blocks, panels):
    rows = panels[0].shape[0]
    return pl.pallas_call(
        chain_kernel,
        out_shape=jax.ShapeDtypeStruct((rows, SIZE), BF16),
        in_specs=[ANY] * (2 * SIDE),
        out_specs=VMEM,
        scratch_shapes=[
            pltpu.VMEM((SIZE, SIZE), BF16),
            pltpu.VMEM((rows // HALF, TABLES, HALF, HALF), BF16),
            pltpu.VMEM((TABLES, HALF, HALF), BF16),
            pltpu.VMEM((TABLES, HALF, HALF), BF16),
            pltpu.SemaphoreType.DMA((SIDE, SIDE)),
            pltpu.SemaphoreType.DMA((SIDE,)),
        ],
        compiler_params=pltpu.CompilerParams(vmem_limit_bytes=16 << 20),
        cost_estimate=cost(14_000_000_000),
        name="chain",
    )(*blocks, *panels)


def final_call(own, pieces, weights):
    rows, cols = weights.shape
    tiles = cols // HALF
    return pl.pallas_call(
        final_kernel,
        out_shape=jax.ShapeDtypeStruct((rows, cols), jnp.int32),
        in_specs=[VMEM] + [ANY] * (SIDE + 1),
        out_specs=ANY,
        scratch_shapes=[
            pltpu.VMEM((2, TABLES, rows, HALF), BF16),
            pltpu.VMEM((2, 2, TABLES, HALF, HALF), BF16),
            pltpu.VMEM((SIZE, cols), BF16),
            pltpu.VMEM((2, 2, 3, HALF, HALF), F32),
            pltpu.VMEM((rows, cols), jnp.int32),
            pltpu.VMEM((rows, cols), jnp.int32),
            pltpu.SemaphoreType.DMA((SIDE, SIDE)),
            pltpu.SemaphoreType.DMA((tiles,)),
            pltpu.SemaphoreType.DMA((tiles,)),
        ],
        compiler_params=pltpu.CompilerParams(vmem_limit_bytes=28 << 20),
        cost_estimate=cost(4_000_000_000),
        name="final",
    )(own, *pieces, weights)


def gather_line(array, axis, lines):
    got = {0: array}
    for shift in (1, 3, 2):
        pairs = [(line[i], line[(i + shift) % SIDE]) for line in lines for i in range(SIDE)]
        got[shift] = lax.ppermute(array, axis, pairs)
    return [got[shift] for shift in range(SIDE)]


def per_device(weights):
    _, cols = weights.shape
    row = lax.axis_index("row")
    panel = weights[:, :PIVOT].astype(BF16)
    strip = weights[:PIVOT, :].astype(BF16)
    panel = lax.all_gather(panel, "col", axis_index_groups=PAIR)[0]
    block = panel[:PIVOT].reshape(SIDE * SIDE, cols)
    message = jnp.concatenate([strip[:PART], block])
    for y in range(1, SIDE):
        sent = jnp.concatenate([strip[y * PART : (y + 1) * PART], block])
        got = lax.ppermute(sent, "row", [(line[0], line[y]) for line in LINE])
        message = jnp.where(row % SIDE == y, got, message)
    panels = gather_line(panel, "col", COL_LINE)
    along_x = gather_line(message, "row", COLUMN)
    quarters = jnp.stack([m[:PART] for m in along_x])
    blocks = jnp.stack([m[PART:].reshape(PIVOT, PIVOT) for m in along_x])
    blocks = gather_line(blocks, "col", COL_LINE)
    pieces = gather_line(quarters, "row", LINE)
    own = chain_call(blocks, panels)
    return final_call(own, pieces, weights)


def solution(mesh):
    placed = (P("row", "col"),)
    return jax.shard_map(
        per_device, mesh=mesh, in_specs=placed, out_specs=P("row", "col"), check_vma=False
    )
```

```python
import jax
import jax.numpy as jnp
from jax import lax
from jax.experimental import pallas as pl
from jax.experimental.pallas import tpu as pltpu
from jax.sharding import PartitionSpec as P

PIVOT = 128
STEPS = 4
SIDE = 4
HALF = 2 * PIVOT
SIZE = STEPS * PIVOT
F32, BF16 = jnp.float32, jnp.bfloat16
RATE = 8.0625
LN2 = 0.6931471805599453
SLACK = 0.004
TABLES = 6
SQUARINGS = 6
LINE = [[SIDE * i + k for k in range(SIDE)] for i in range(SIDE)]
COLUMN = [[SIDE * k + i for k in range(SIDE)] for i in range(SIDE)]
COL_LINE = [[2 * k + c for k in range(SIDE)] for c in range(2)]
PAIR = [[2 * k, 2 * k + 1] for k in range(SIDE)]


def encode(value):
    far = value >= BF16(33.0)
    a = value - jnp.where(far, BF16(33.0), BF16(1.0))
    scale = jnp.exp2(BF16(125.0) - BF16(8.0) * a) * jnp.exp2(BF16(-0.0625) * a)
    zero = jnp.zeros_like(scale)
    lo = jnp.where(far, zero, scale)
    t5 = jnp.where(far, scale * BF16(2.0**-12), zero)
    mid = jnp.where(value >= BF16(17.0), lo, zero)
    t1 = lo * BF16(2.0**-66)
    t4 = t1 * BF16(2.0**-62)
    t3 = t5 * BF16(2.0**-118)
    return t1, lo, t3, t4, t5, mid * BF16(2.0**123)


def decode(s1, s2, s3):
    near = s1 >= 2.0**-59.4
    middle = s2 >= 2.0**-121
    s = jnp.where(near, s1, jnp.where(middle, s2, s3))
    p1, p2, p3 = (p / RATE - SLACK + 2.0 for p in (118.0, 250.0, 496.0))
    p = jnp.where(near, p1, jnp.where(middle, p2, p3))
    return jnp.ceil(p - jnp.log(s) * (1.0 / (RATE * LN2)))


def dot(left, right):
    return jnp.dot(left, right, preferred_element_type=F32)


CHUNK = 32


def sums(left, right, rows, cols):
    def l(*tables):
        return jnp.concatenate([left[t, rows, :] for t in tables], axis=1)

    def r(*tables):
        return jnp.concatenate([right[t, :, cols] for t in tables], axis=0)

    return dot(l(0), r(0)), dot(l(3, 2, 1), r(2, 3, 1)), dot(l(1, 4, 5), r(4, 1, 5))


def lower(ref, rows, cols, windows):
    for i in range(0, windows[0].shape[0], CHUNK):
        at = slice(rows + i, rows + i + CHUNK)
        new = decode(*(w[i : i + CHUNK] for w in windows))
        ref[at, cols] = jnp.minimum(ref[at, cols].astype(F32), new).astype(BF16)


def encode_rows(ref, rows, cols, count, to, at=0):
    for i in range(0, count, CHUNK):
        for t, table in enumerate(encode(ref[rows + i : rows + i + CHUNK, cols])):
            to[t, at + i : at + i + CHUNK, :] = table


ALL = slice(0, HALF)
P_, Q_ = slice(0, HALF), slice(HALF, SIZE)


def square(x_ref, at, tab_ref):
    cols = slice(at, at + HALF)
    lower(x_ref, at, cols, sums(tab_ref, tab_ref, ALL, ALL))
    encode_rows(x_ref, at, cols, HALF, tab_ref)


def close(x_ref, at, tab_ref):
    def body(_, carry):
        square(x_ref, at, tab_ref)
        return carry

    encode_rows(x_ref, at, slice(at, at + HALF), HALF, tab_ref)
    lax.fori_loop(0, SQUARINGS, body, 0)


def multiply(ref, cols, source, source_cols, left, right_ref, r):
    encode_rows(source, r, source_cols, HALF, left)
    lower(ref, r, cols, sums(left, right_ref, ALL, ALL))


def chain_kernel(*refs):
    blocks, panels = refs[:SIDE], refs[SIDE : 2 * SIDE]
    own_ref, x_ref, left_ref, right_ref, tab_ref, block_sem, panel_sem = refs[2 * SIDE :]
    rows = own_ref.shape[0]
    first = lax.axis_index("row") // SIDE + 2 * SIDE - lax.axis_index("col") // 2
    block_copies, panel_copies = [], []
    for shift in range(SIDE):
        col = pl.ds(pl.multiple_of(lax.rem(first + shift, SIDE) * PIVOT, PIVOT), PIVOT)
        for other in range(SIDE):
            to = x_ref.at[other * PIVOT : (other + 1) * PIVOT, col]
            block_copies.append(pltpu.make_async_copy(blocks[shift].at[other], to, block_sem.at[shift, other]))
        panel_copies.append(pltpu.make_async_copy(panels[shift], own_ref.at[:, col], panel_sem.at[shift]))
    for copy in block_copies + panel_copies:
        copy.start()
    for copy in block_copies:
        copy.wait()
    halves = range(0, rows, HALF)
    close(x_ref, 0, tab_ref.at[0])
    multiply(x_ref, P_, x_ref, P_, left_ref.at[0], tab_ref.at[0], HALF)
    encode_rows(x_ref, 0, Q_, HALF, right_ref)
    multiply(x_ref, Q_, x_ref, P_, left_ref.at[1], right_ref, HALF)
    for copy in panel_copies:
        copy.wait()
    work = [(cols, table, r) for cols, table in ((P_, tab_ref.at[0]), (Q_, right_ref)) for r in halves]
    encode_rows(x_ref, HALF, Q_, HALF, tab_ref.at[1])
    for n in range(SQUARINGS):
        if n < len(work):
            cols, table, r = work[n]
            multiply(own_ref, cols, own_ref, P_, left_ref.at[n % 2], table, r)
        square(x_ref, HALF, tab_ref.at[1])
    for cols, table, r in work[SQUARINGS:]:
        multiply(own_ref, cols, own_ref, P_, left_ref.at[0], table, r)
    encode_rows(x_ref, HALF, P_, HALF, right_ref)
    for n, r in enumerate(halves):
        multiply(own_ref, Q_, own_ref, Q_, left_ref.at[n % 2], tab_ref.at[1], r)
    for n, r in enumerate(halves):
        multiply(own_ref, P_, own_ref, Q_, left_ref.at[n % 2], right_ref, r)


def final_kernel(own_ref, *refs):
    pieces = refs[:SIDE]
    weights_ref, out_hbm, left_ref, right_ref, sums_ref, out_ref, sem = refs[SIDE:]
    rows, total = weights_ref.shape
    row, col = lax.axis_index("row"), lax.axis_index("col")
    starts = [pl.multiple_of(lax.rem(row % SIDE + SIDE - n, SIDE) * HALF, HALF) for n in range(SIDE)]
    stores = [
        pltpu.make_async_copy(out_ref.at[n], out_hbm.at[:, pl.ds(starts[n], HALF)], sem.at[n]) for n in range(SIDE)
    ]
    for chunk in range(2):
        encode_rows(own_ref, 0, slice(chunk * HALF, (chunk + 1) * HALF), rows, left_ref.at[chunk])

    def finish(n, r, slot):
        diagonal = row * rows + r - col * total - starts[n]
        for i in range(0, HALF, CHUNK):
            at, to = slice(i, i + CHUNK), slice(r + i, r + i + CHUNK)
            new = decode(*(jnp.maximum(sums_ref[slot, 0, w, at, :], sums_ref[slot, 1, w, at, :]) for w in range(3)))
            old = weights_ref[to, pl.ds(starts[n], HALF)].astype(F32)
            best = jnp.minimum(old, new).astype(jnp.int32)
            down = lax.broadcasted_iota(jnp.int32, best.shape, 0)
            across = lax.broadcasted_iota(jnp.int32, best.shape, 1)
            out_ref[n, to, :] = jnp.where(across - down == diagonal + i, 0, best)
        if r + HALF == rows:
            stores[n].start()

    units = [(n, r) for n in range(SIDE) for r in range(0, rows, HALF)]
    for u, (n, r) in enumerate(units):
        if r == 0:
            for k in range(SIDE):
                encode_rows(pieces[n].at[k], 0, ALL, PIVOT, right_ref.at[n % 2, k // 2], (k % 2) * PIVOT)
        for chunk in range(2):
            at = slice(r, r + HALF)
            for w, value in enumerate(sums(left_ref.at[chunk], right_ref.at[n % 2, chunk], at, ALL)):
                sums_ref[u % 2, chunk, w] = value
        if u:
            finish(*units[u - 1], (u - 1) % 2)
    finish(*units[-1], (len(units) - 1) % 2)
    for copy in stores:
        copy.wait()


VMEM = pl.BlockSpec(memory_space=pltpu.VMEM)
ANY = pl.BlockSpec(memory_space=pl.ANY)


def cost(flops):
    return pl.CostEstimate(flops=flops, bytes_accessed=2_000_000, transcendentals=0)


def chain_call(blocks, panels):
    rows = panels[0].shape[0]
    return pl.pallas_call(
        chain_kernel,
        out_shape=jax.ShapeDtypeStruct((rows, SIZE), BF16),
        in_specs=[ANY] * (2 * SIDE),
        out_specs=VMEM,
        scratch_shapes=[
            pltpu.VMEM((SIZE, SIZE), BF16),
            pltpu.VMEM((2, TABLES, HALF, HALF), BF16),
            pltpu.VMEM((TABLES, HALF, HALF), BF16),
            pltpu.VMEM((2, TABLES, HALF, HALF), BF16),
            pltpu.SemaphoreType.DMA((SIDE, SIDE)),
            pltpu.SemaphoreType.DMA((SIDE,)),
        ],
        compiler_params=pltpu.CompilerParams(vmem_limit_bytes=16 << 20),
        cost_estimate=cost(14_000_000_000),
        name="chain",
    )(*blocks, *panels)


def final_call(own, pieces, weights):
    rows, cols = weights.shape
    return pl.pallas_call(
        final_kernel,
        out_shape=jax.ShapeDtypeStruct((rows, cols), jnp.int32),
        in_specs=[VMEM] * (SIDE + 2),
        out_specs=ANY,
        scratch_shapes=[
            pltpu.VMEM((2, TABLES, rows, HALF), BF16),
            pltpu.VMEM((2, 2, TABLES, HALF, HALF), BF16),
            pltpu.VMEM((2, 2, 3, HALF, HALF), F32),
            pltpu.VMEM((SIDE, rows, HALF), jnp.int32),
            pltpu.SemaphoreType.DMA((SIDE,)),
        ],
        compiler_params=pltpu.CompilerParams(vmem_limit_bytes=28 << 20),
        cost_estimate=cost(4_000_000_000),
        name="final",
    )(own, *pieces, weights)


def gather_line(array, axis, lines):
    got = {0: array}
    for shift in (1, 3, 2):
        pairs = [(line[i], line[(i + shift) % SIDE]) for line in lines for i in range(SIDE)]
        got[shift] = lax.ppermute(array, axis, pairs)
    return [got[shift] for shift in range(SIDE)]


def per_device(weights):
    row = lax.axis_index("row")
    strip = lax.optimization_barrier(weights[:PIVOT, :]).astype(BF16)
    block = lax.all_gather(strip[:, :PIVOT], "col", axis_index_groups=PAIR)[0]
    panel = lax.optimization_barrier(weights[:, :PIVOT]).astype(BF16)
    panel = lax.all_gather(panel, "col", axis_index_groups=PAIR)[0]
    message = jnp.concatenate([strip[:, :HALF], block], axis=1)
    for y in range(1, SIDE):
        sent = jnp.concatenate([strip[:, y * HALF : (y + 1) * HALF], block], axis=1)
        got = lax.ppermute(sent, "row", [(line[0], line[y]) for line in LINE])
        message = jnp.where(row % SIDE == y, got, message)
    panels = gather_line(panel, "col", COL_LINE)
    along_x = gather_line(message, "row", COLUMN)
    quarters = jnp.stack([m[:, :HALF] for m in along_x])
    blocks = jnp.stack([m[:, HALF:] for m in along_x])
    blocks = gather_line(blocks, "col", COL_LINE)
    pieces = gather_line(quarters, "row", LINE)
    own = chain_call(blocks, panels)
    return final_call(own, pieces, weights)


def solution(mesh):
    placed = (P("row", "col"),)
    return jax.shard_map(
        per_device, mesh=mesh, in_specs=placed, out_specs=P("row", "col"), check_vma=False
    )
```

```python
import jax
import jax.numpy as jnp
from jax import lax
from jax.experimental import pallas as pl
from jax.experimental.pallas import tpu as pltpu
from jax.sharding import PartitionSpec as P

PIVOT = 128
STEPS = 4
SIDE = 4
HALF = 2 * PIVOT
SIZE = STEPS * PIVOT
F32, BF16 = jnp.float32, jnp.bfloat16
RATE = 8.0625
LN2 = 0.6931471805599453
SLACK = 0.004
TABLES = 6
SQUARINGS = 6
LINE = [[SIDE * i + k for k in range(SIDE)] for i in range(SIDE)]
COLUMN = [[SIDE * k + i for k in range(SIDE)] for i in range(SIDE)]
COL_LINE = [[2 * k + c for k in range(SIDE)] for c in range(2)]
PAIR = [[2 * k, 2 * k + 1] for k in range(SIDE)]


def encode(value):
    far = value >= BF16(33.0)
    a = value - jnp.where(far, BF16(33.0), BF16(1.0))
    scale = jnp.exp2(BF16(125.0) - BF16(8.0) * a) * jnp.exp2(BF16(-0.0625) * a)
    zero = jnp.zeros_like(scale)
    lo = jnp.where(far, zero, scale)
    t5 = jnp.where(far, scale * BF16(2.0**-12), zero)
    mid = jnp.where(value >= BF16(17.0), lo, zero)
    t1 = lo * BF16(2.0**-66)
    t4 = t1 * BF16(2.0**-62)
    t3 = t5 * BF16(2.0**-118)
    return t1, lo, t3, t4, t5, mid * BF16(2.0**123)


def decode(s1, s2, s3):
    near = s1 >= 2.0**-59.4
    middle = s2 >= 2.0**-121
    s = jnp.where(near, s1, jnp.where(middle, s2, s3))
    p1, p2, p3 = (p / RATE - SLACK + 2.0 for p in (118.0, 250.0, 496.0))
    p = jnp.where(near, p1, jnp.where(middle, p2, p3))
    return jnp.ceil(p - jnp.log(s) * (1.0 / (RATE * LN2)))


def dot(left, right):
    return jnp.dot(left, right, preferred_element_type=F32)


CHUNK = 32


def sums(left, right, rows, cols):
    def l(*tables):
        return jnp.concatenate([left[t, rows, :] for t in tables], axis=1)

    def r(*tables):
        return jnp.concatenate([right[t, :, cols] for t in tables], axis=0)

    return dot(l(0), r(0)), dot(l(3, 2, 1), r(2, 3, 1)), dot(l(1, 4, 5), r(4, 1, 5))


def lower(ref, rows, cols, windows):
    for i in range(0, windows[0].shape[0], CHUNK):
        at = slice(rows + i, rows + i + CHUNK)
        new = decode(*(w[i : i + CHUNK] for w in windows))
        ref[at, cols] = jnp.minimum(ref[at, cols].astype(F32), new).astype(BF16)


def encode_rows(ref, rows, cols, count, to, at=0):
    for i in range(0, count, CHUNK):
        for t, table in enumerate(encode(ref[rows + i : rows + i + CHUNK, cols])):
            to[t, at + i : at + i + CHUNK, :] = table


ALL = slice(0, HALF)
P_, Q_ = slice(0, HALF), slice(HALF, SIZE)


def square(x_ref, at, tab_ref):
    cols = slice(at, at + HALF)
    parts = [sums(tab_ref, tab_ref, slice(r, r + PIVOT), ALL) for r in (0, PIVOT)]
    for n, part in enumerate(parts):
        lower(x_ref, at + n * PIVOT, cols, part)
        encode_rows(x_ref, at + n * PIVOT, cols, PIVOT, tab_ref, n * PIVOT)


def close(x_ref, at, tab_ref):
    def body(_, carry):
        square(x_ref, at, tab_ref)
        return carry

    encode_rows(x_ref, at, slice(at, at + HALF), HALF, tab_ref)
    lax.fori_loop(0, SQUARINGS, body, 0)


def multiply(ref, cols, source, source_cols, left, right_ref, r):
    encode_rows(source, r, source_cols, HALF, left)
    lower(ref, r, cols, sums(left, right_ref, ALL, ALL))


def chain_kernel(*refs):
    blocks, panels = refs[:SIDE], refs[SIDE : 2 * SIDE]
    own_ref, x_ref, left_ref, right_ref, tab_ref, block_sem, panel_sem = refs[2 * SIDE :]
    rows = own_ref.shape[0]
    first = lax.axis_index("row") // SIDE + 2 * SIDE - lax.axis_index("col") // 2
    block_copies, panel_copies = [], []
    for shift in range(SIDE):
        col = pl.ds(pl.multiple_of(lax.rem(first + shift, SIDE) * PIVOT, PIVOT), PIVOT)
        for other in range(SIDE):
            to = x_ref.at[other * PIVOT : (other + 1) * PIVOT, col]
            block_copies.append(pltpu.make_async_copy(blocks[shift].at[other], to, block_sem.at[shift, other]))
        panel_copies.append(pltpu.make_async_copy(panels[shift], own_ref.at[:, col], panel_sem.at[shift]))
    for copy in block_copies + panel_copies:
        copy.start()
    for copy in block_copies:
        copy.wait()
    halves = range(0, rows, HALF)
    close(x_ref, 0, tab_ref.at[0])
    multiply(x_ref, P_, x_ref, P_, left_ref.at[0], tab_ref.at[0], HALF)
    encode_rows(x_ref, 0, Q_, HALF, right_ref)
    multiply(x_ref, Q_, x_ref, P_, left_ref.at[1], right_ref, HALF)
    for copy in panel_copies:
        copy.wait()
    work = [(cols, table, r) for cols, table in ((P_, tab_ref.at[0]), (Q_, right_ref)) for r in halves]
    encode_rows(x_ref, HALF, Q_, HALF, tab_ref.at[1])
    for n in range(SQUARINGS):
        if n < len(work):
            cols, table, r = work[n]
            multiply(own_ref, cols, own_ref, P_, left_ref.at[n % 2], table, r)
        square(x_ref, HALF, tab_ref.at[1])
    for cols, table, r in work[SQUARINGS:]:
        multiply(own_ref, cols, own_ref, P_, left_ref.at[0], table, r)
    encode_rows(x_ref, HALF, P_, HALF, right_ref)
    for n, r in enumerate(halves):
        multiply(own_ref, Q_, own_ref, Q_, left_ref.at[n % 2], tab_ref.at[1], r)
    for n, r in enumerate(halves):
        multiply(own_ref, P_, own_ref, Q_, left_ref.at[n % 2], right_ref, r)


def final_kernel(own_ref, *refs):
    pieces = refs[:SIDE]
    weights_ref, out_hbm, left_ref, right_ref, sums_ref, out_ref, sem = refs[SIDE:]
    rows, total = weights_ref.shape
    row, col = lax.axis_index("row"), lax.axis_index("col")
    starts = [pl.multiple_of(lax.rem(row % SIDE + SIDE - n, SIDE) * HALF, HALF) for n in range(SIDE)]
    stores = [
        pltpu.make_async_copy(out_ref.at[n], out_hbm.at[:, pl.ds(starts[n], HALF)], sem.at[n]) for n in range(SIDE)
    ]
    for chunk in range(2):
        encode_rows(own_ref, 0, slice(chunk * HALF, (chunk + 1) * HALF), rows, left_ref.at[chunk])

    def finish(n, r, slot):
        diagonal = row * rows + r - col * total - starts[n]
        for i in range(0, HALF, CHUNK):
            at, to = slice(i, i + CHUNK), slice(r + i, r + i + CHUNK)
            new = decode(*(jnp.maximum(sums_ref[slot, 0, w, at, :], sums_ref[slot, 1, w, at, :]) for w in range(3)))
            old = weights_ref[to, pl.ds(starts[n], HALF)].astype(F32)
            best = jnp.minimum(old, new).astype(jnp.int32)
            down = lax.broadcasted_iota(jnp.int32, best.shape, 0)
            across = lax.broadcasted_iota(jnp.int32, best.shape, 1)
            out_ref[n, to, :] = jnp.where(across - down == diagonal + i, 0, best)
        if r + HALF == rows:
            stores[n].start()

    units = [(n, r) for n in range(SIDE) for r in range(0, rows, HALF)]
    for u, (n, r) in enumerate(units):
        if r == 0:
            for k in range(SIDE):
                encode_rows(pieces[n].at[k], 0, ALL, PIVOT, right_ref.at[n % 2, k // 2], (k % 2) * PIVOT)
        for chunk in range(2):
            at = slice(r, r + HALF)
            for w, value in enumerate(sums(left_ref.at[chunk], right_ref.at[n % 2, chunk], at, ALL)):
                sums_ref[u % 2, chunk, w] = value
        if u:
            finish(*units[u - 1], (u - 1) % 2)
    finish(*units[-1], (len(units) - 1) % 2)
    for copy in stores:
        copy.wait()


VMEM = pl.BlockSpec(memory_space=pltpu.VMEM)
ANY = pl.BlockSpec(memory_space=pl.ANY)


def cost(flops):
    return pl.CostEstimate(flops=flops, bytes_accessed=2_000_000, transcendentals=0)


def chain_call(blocks, panels):
    rows = panels[0].shape[0]
    return pl.pallas_call(
        chain_kernel,
        out_shape=jax.ShapeDtypeStruct((rows, SIZE), BF16),
        in_specs=[ANY] * (2 * SIDE),
        out_specs=VMEM,
        scratch_shapes=[
            pltpu.VMEM((SIZE, SIZE), BF16),
            pltpu.VMEM((2, TABLES, HALF, HALF), BF16),
            pltpu.VMEM((TABLES, HALF, HALF), BF16),
            pltpu.VMEM((2, TABLES, HALF, HALF), BF16),
            pltpu.SemaphoreType.DMA((SIDE, SIDE)),
            pltpu.SemaphoreType.DMA((SIDE,)),
        ],
        compiler_params=pltpu.CompilerParams(vmem_limit_bytes=16 << 20),
        cost_estimate=cost(14_000_000_000),
        name="chain",
    )(*blocks, *panels)


def final_call(own, pieces, weights):
    rows, cols = weights.shape
    return pl.pallas_call(
        final_kernel,
        out_shape=jax.ShapeDtypeStruct((rows, cols), jnp.int32),
        in_specs=[VMEM] * (SIDE + 2),
        out_specs=ANY,
        scratch_shapes=[
            pltpu.VMEM((2, TABLES, rows, HALF), BF16),
            pltpu.VMEM((2, 2, TABLES, HALF, HALF), BF16),
            pltpu.VMEM((2, 2, 3, HALF, HALF), F32),
            pltpu.VMEM((SIDE, rows, HALF), jnp.int32),
            pltpu.SemaphoreType.DMA((SIDE,)),
        ],
        compiler_params=pltpu.CompilerParams(vmem_limit_bytes=28 << 20),
        cost_estimate=cost(4_000_000_000),
        name="final",
    )(own, *pieces, weights)


def gather_line(array, axis, lines):
    got = {0: array}
    for shift in (1, 3, 2):
        pairs = [(line[i], line[(i + shift) % SIDE]) for line in lines for i in range(SIDE)]
        got[shift] = lax.ppermute(array, axis, pairs)
    return [got[shift] for shift in range(SIDE)]


def per_device(weights):
    row = lax.axis_index("row")
    strip = lax.optimization_barrier(weights[:PIVOT, :]).astype(BF16)
    roots = [(line[0] * lax.axis_size("col") + a, line[0] * lax.axis_size("col") + b) for line in LINE for a, b in PAIR]
    block = lax.ppermute(strip[:, :PIVOT], ("row", "col"), roots)
    block = jnp.where(lax.axis_index("col") % 2 == 0, strip[:, :PIVOT], block)
    panel = lax.optimization_barrier(weights[:, :PIVOT]).astype(BF16)
    panel = lax.all_gather(panel, "col", axis_index_groups=PAIR)[0]
    message = jnp.concatenate([strip[:, :HALF], block], axis=1)
    for y in (3, 2, 1):
        sent = jnp.concatenate([strip[:, y * HALF : (y + 1) * HALF], block], axis=1)
        got = lax.ppermute(sent, "row", [(line[0], line[y]) for line in LINE])
        message = jnp.where(row % SIDE == y, got, message)
    panels = gather_line(panel, "col", COL_LINE)
    along_x = gather_line(message, "row", COLUMN)
    quarters = jnp.stack([m[:, :HALF] for m in along_x])
    blocks = jnp.stack([m[:, HALF:] for m in along_x])
    blocks = gather_line(blocks, "col", COL_LINE)
    pieces = gather_line(quarters, "row", LINE)
    own = chain_call(blocks, panels)
    return final_call(own, pieces, weights)


def solution(mesh):
    placed = (P("row", "col"),)
    return jax.shard_map(
        per_device, mesh=mesh, in_specs=placed, out_specs=P("row", "col"), check_vma=False
    )
```
